32 devices in a mesh: groups: 2 (over y), tx: 4 (over z), ty: 2 (over x), ka: 2 (over core).
Axes of the slice: x: 2, y: 2, z: 4, core: 2. Of those that a mesh axis runs over, the one named last changes fastest.
Arguments:
- mask_raster: float32 [2048, 512], P(('groups', 'tx'), 'ty'), parts along dimension 0, may hold values from 0 to 1
- frag_rows: int32 [8, 2, 512], P(('groups', 'tx'), 'ty'), parts along dimension 0, may hold values from 8 to 215
- frag_cols: int32 [8, 2, 512], P(('groups', 'tx'), 'ty'), parts along dimension 0, may hold values from 8 to 215
- frag_length: int32 [8, 2, 512], P(('groups', 'tx'), 'ty'), parts along dimension 0, may hold values from 4 to 32
- frag_orient: int32 [8, 2, 512], P(('groups', 'tx'), 'ty'), parts along dimension 0, may hold values from 0 to 1
- frag_moves: int32 [8, 2, 2, 512], P(('groups', 'tx'), 'ty'), parts along dimension 0, may hold values from -4 to 4
- site_rows: int32 [8, 2, 2048], P(('groups', 'tx'), 'ty'), parts along dimension 0, may hold values from 1 to 254
- site_cols: int32 [8, 2, 2048], P(('groups', 'tx'), 'ty'), parts along dimension 0, may hold values from 1 to 254
- spectra: float32 [16, 2, 128, 128], P('ka'), may hold values from -24 to 24
- weights: float32 [16], P('ka'), may hold values from 0.05 to 1
- tolerance: int32 [2], replicated, may hold values from 1 to 16
Outputs:
- intensity: float32 [2048, 512], P(('groups', 'tx'), 'ty'), parts along dimension 0
- corrected_mask: float32 [2048, 512], P(('groups', 'tx'), 'ty'), parts along dimension 0
- edge_errors: float32 [8, 2, 2, 2048], P(('groups', 'tx'), 'ty'), parts along dimension 0
- peak_error: float32 [4], P('groups'), parts along dimension 0
- converged_share: float32 [4], P('groups'), parts along dimension 0
The draws below stay inside these ranges and needn't reach their ends.
There are 2 independent parts, one for each index of `groups`. The reference program is written for one: setup_inputs(seed, part) draws one part's arguments, and reference() takes and returns one part's arrays. A program takes and returns all parts, laid end to end along the dimension named above; an argument that names none is the same for every part. Nothing has to cross between parts.
All inputs are finite; a program needn't handle non-finite values.
Results may differ from the reference program's by a relative error of at most 0.0003.
Values sent between devices are 32-bit elements; how exact they have to be, the bound alone decides.
No kernel may reach another device: no remote copies, remote signals or barrier semaphores. Data moves between devices by JAX's collectives and lax.ppermute only.
A program may use at most 64 MiB of HBM per device.

```python
import math
import jax
import jax.numpy as jnp
from jax import lax

TILE = 256
HALO = 128
BAND = 128
KERNELS = 16
NFRAG = 512
SITES = 2048
ITERS = 2
ROWS = 1024
COLS = 512
N_TX = 4
N_TY = 2


def draw_spectra(key, part):
    shape = (KERNELS, 2, BAND, BAND)
    scale = (TILE + 2 * HALO) / BAND
    values = jnp.clip(jax.random.normal(key, shape, jnp.float32), -6.0, 6.0)
    first = jnp.arange(BAND)[:, None] == BAND // 2
    second = jnp.arange(BAND)[None, :] == BAND // 2
    factor = jnp.where(first & second, 0.02, 1.0)
    return (values * scale * factor[None, None]).astype(jnp.float32)


def plant(drawn, key, low, top_value):
    spot = [jax.random.randint(jax.random.fold_in(key, axis), (), 0, length) for axis, length in enumerate(drawn.shape)]
    main_axis = drawn.shape.index(max(drawn.shape))
    neighbour = spot[:main_axis] + [(spot[main_axis] + 1) % drawn.shape[main_axis]] + spot[main_axis + 1:]
    return drawn.at[tuple(spot)].set(low).at[tuple(neighbour)].set(top_value)


def steps_of(stream_key, dims, pieces, low, largest):
    loudness = 1.0
    for dim, shards_of in pieces:
        heights = jax.random.uniform(jax.random.fold_in(jax.random.fold_in(stream_key, 6), dim), (shards_of,), jnp.float32, low / len(pieces), largest / len(pieces))
        loudness = loudness * jnp.repeat(jnp.exp(heights), dims[dim] // shards_of).reshape((-1,) + (1,) * (len(dims) - 1 - dim))
    return loudness


def setup_inputs(seed: int = 0, part: int = 0) -> dict:
    key_list = jax.random.split(jax.random.key(seed), 12)
    part_keys = jax.random.split(jax.random.fold_in(key_list[11], part), 12)
    mask_raster = jnp.clip(1.0 * jax.random.uniform(part_keys[0], (ROWS, COLS), jnp.float32) ** steps_of(part_keys[0], (ROWS, COLS), ((0, 4), (1, 2)), -0.2, 0.2), 0.0, 1.0)
    frag_rows = plant(jax.random.randint(part_keys[1], (N_TX, N_TY, NFRAG), 8, TILE - 40), jax.random.fold_in(part_keys[1], 1), 8, (TILE - 40) - 1).astype(jnp.int32)
    frag_cols = plant(jax.random.randint(part_keys[2], (N_TX, N_TY, NFRAG), 8, TILE - 40), jax.random.fold_in(part_keys[2], 1), 8, (TILE - 40) - 1).astype(jnp.int32)
    frag_length = plant(jax.random.randint(part_keys[3], (N_TX, N_TY, NFRAG), 4, 33), jax.random.fold_in(part_keys[3], 1), 4, 32).astype(jnp.int32)
    frag_orient = plant(jax.random.randint(part_keys[4], (N_TX, N_TY, NFRAG), 0, 2), jax.random.fold_in(part_keys[4], 1), 0, 1).astype(jnp.int32)
    frag_moves = plant(jax.random.randint(part_keys[5], (N_TX, N_TY, ITERS, NFRAG), -4, 5), jax.random.fold_in(part_keys[5], 1), -4, 4).astype(jnp.int32)
    site_rows = plant(jax.random.randint(part_keys[6], (N_TX, N_TY, SITES), 1, TILE - 1), jax.random.fold_in(part_keys[6], 1), 1, (TILE - 1) - 1).astype(jnp.int32)
    site_cols = plant(jax.random.randint(part_keys[7], (N_TX, N_TY, SITES), 1, TILE - 1), jax.random.fold_in(part_keys[7], 1), 1, (TILE - 1) - 1).astype(jnp.int32)
    spectra = draw_spectra(jax.random.fold_in(key_list[11], 71), part)
    weights = jnp.clip(jnp.exp(math.log(1.0) - 2.9957323 * jax.random.uniform(key_list[9], (KERNELS,), jnp.float32) ** steps_of(key_list[9], (KERNELS,), ((0, 2),), -0.2, 0.2)), 0.05, 1.0)
    tolerance = jax.random.randint(key_list[10], (ITERS,), 1, 17).astype(jnp.int32)
    return {"mask_raster": mask_raster, "frag_rows": frag_rows, "frag_cols": frag_cols, "frag_length": frag_length, "frag_orient": frag_orient, "frag_moves": frag_moves, "site_rows": site_rows, "site_cols": site_cols, "spectra": spectra, "weights": weights, "tolerance": tolerance}


LEVEL = 0.4
SLOPE_FLOOR = 0.05
SHARPNESS = 8.0

def strip_sum(row_start, col_start, frag_len, orient, shift, extent):
    lower = jnp.minimum(shift, 0)
    upper = jnp.maximum(shift, 0)
    along_rows = orient == 0
    row_low = jnp.where(along_rows, row_start, row_start + lower)
    row_high = jnp.where(along_rows, row_start + frag_len, row_start + upper)
    col_low = jnp.where(along_rows, col_start + lower, col_start)
    col_high = jnp.where(along_rows, col_start + upper, col_start + frag_len)
    position = jnp.arange(extent, dtype=jnp.int32)
    signs = jnp.sign(shift).astype(jnp.float32)
    row_select = ((position[:, None] >= row_low[None, :]) & (position[:, None] < row_high[None, :])).astype(jnp.float32) * signs[None, :]
    col_select = ((position[None, :] >= col_low[:, None]) & (position[None, :] < col_high[:, None])).astype(jnp.float32)
    return jnp.dot(row_select.astype(jnp.bfloat16), col_select.astype(jnp.bfloat16), preferred_element_type=jnp.float32)

def edge_error(image, rows_at, cols_at):
    flat = image.reshape(-1)
    width = image.shape[1]

    def sample(delta_row, delta_col):
        return flat[(rows_at + delta_row) * width + cols_at + delta_col]
    center = sample(0, 0)
    grad_rows = (sample(1, 0) - sample(-1, 0)) * 0.5
    grad_cols = (sample(0, 1) - sample(0, -1)) * 0.5
    slope = jnp.sqrt(grad_rows * grad_rows + grad_cols * grad_cols)
    return (center - LEVEL) / jnp.maximum(slope, SLOPE_FLOOR)

def reference(mask_raster, frag_rows, frag_cols, frag_length, frag_orient, frag_moves, site_rows, site_cols, spectra, weights, tolerance):
    tiles_x = mask_raster.shape[0] // TILE
    tiles_y = mask_raster.shape[1] // TILE
    count = tiles_x * tiles_y
    ext_size = TILE + 2 * HALO
    freq = (jnp.arange(BAND, dtype=jnp.int32) - BAND // 2) % ext_size
    kernel_spec = spectra[:, 0] + 1j * spectra[:, 1]
    current = mask_raster
    flat_rows = frag_rows.reshape(count, NFRAG)
    flat_cols = frag_cols.reshape(count, NFRAG)
    flat_len = frag_length.reshape(count, NFRAG)
    flat_orient = frag_orient.reshape(count, NFRAG)
    errors_all = []
    peaks = []
    shares = []
    images = None
    for iteration in range(ITERS):
        flat_moves = frag_moves[:, :, iteration, :].reshape(count, NFRAG)
        strips = lax.map(lambda items: strip_sum(items[0], items[1], items[2], items[3], items[4], TILE), (flat_rows, flat_cols, flat_len, flat_orient, flat_moves))
        region = strips.reshape(tiles_x, tiles_y, TILE, TILE).transpose(0, 2, 1, 3).reshape(tiles_x * TILE, tiles_y * TILE)
        current = jnp.clip(current + region, 0.0, 1.0)
        padded = jnp.pad(current, HALO)

        def image_tile(number):
            first = (number // tiles_y * TILE).astype(jnp.int32)
            second = (number % tiles_y * TILE).astype(jnp.int32)
            window = lax.dynamic_slice(padded, (first, second), (ext_size, ext_size))
            spectrum = jnp.fft.fft2(window)
            kept = spectrum[freq][:, freq]
            product = kernel_spec * kept[None]
            full = jnp.zeros((product.shape[0], ext_size, ext_size), product.dtype)
            full = full.at[:, freq[:, None], freq[None, :]].set(product)
            field = jnp.fft.ifft2(full, axes=(1, 2))[:, HALO:HALO + TILE, HALO:HALO + TILE]
            return lax.optimization_barrier(jnp.sum(weights[:, None, None] * (field.real * field.real + field.imag * field.imag), axis=0))
        images = lax.map(image_tile, jnp.arange(count, dtype=jnp.int32))
        errors_now = jax.vmap(edge_error)(images, site_rows.reshape(count, SITES), site_cols.reshape(count, SITES))
        errors_all.append(errors_now.reshape(tiles_x, tiles_y, SITES))
        peaks.append(jnp.max(jnp.abs(errors_now)))
        limit = tolerance[iteration].astype(jnp.float32) / 8.0
        shares.append(jnp.mean(jax.nn.sigmoid(SHARPNESS * (limit - jnp.abs(errors_now)))))
    intensity = images.reshape(tiles_x, tiles_y, TILE, TILE).transpose(0, 2, 1, 3).reshape(tiles_x * TILE, tiles_y * TILE)
    edge_errors = jnp.stack(errors_all, axis=2)
    return (intensity, current, edge_errors, jnp.stack(peaks), jnp.stack(shares))
```

```python
import functools
import math

import jax
import jax.numpy as jnp
import numpy as np
from jax import lax
from jax.experimental import pallas as pl
from jax.experimental.pallas import tpu as pltpu
from jax.sharding import PartitionSpec as P

HALO = 128
BAND = 128
ITERS = 2

LEVEL = 0.4
SLOPE_FLOOR = 0.05
SHARPNESS = 8.0

F32 = jnp.float32
BF16 = jnp.bfloat16
VMEM = pltpu.MemorySpace.VMEM
SMEM = pltpu.MemorySpace.SMEM
PAD_ROWS = 16
LIMIT = pltpu.CompilerParams(vmem_limit_bytes=24 * 1024 * 1024)


def terms(x):
    high = x.astype(BF16)
    rest = x - high.astype(F32)
    mid = rest.astype(BF16)
    return high, mid, (rest - mid.astype(F32)).astype(BF16)


def table_terms(table):
    out = []
    for _ in range(3):
        part = table.astype(np.float32).astype(BF16)
        out.append(part)
        table = table - part.astype(np.float64)
    return out


@functools.lru_cache(maxsize=None)
def tables(tile):
    ext = tile + 2 * HALO
    half = BAND // 2
    rows = (BAND + 1 + PAD_ROWS - 1) // PAD_ROWS * PAD_ROWS
    step = 2.0 * math.pi / ext
    place = np.arange(ext) - (ext - 1) / 2
    freq = np.arange(BAND) - half

    def angle(freqs, places):
        return freqs[:, None] * places[None, :] * step

    forward_rows = np.zeros((rows, ext))
    forward_rows[: half + 1] = np.cos(angle(np.arange(half + 1), place))
    forward_rows[half + 1 : BAND + 1] = -np.sin(angle(np.arange(1, half + 1), place))
    turn = angle(place, freq)
    forward_cols = np.concatenate([np.cos(turn), np.sin(turn)], axis=1)
    expand = np.zeros((2 * BAND, rows))
    for index, f in enumerate(freq):
        expand[index, abs(f)] = 1.0
        if f != 0:
            expand[BAND + index, half + abs(f)] = np.sign(f)
    inner = angle(np.arange(tile // 2) + 0.5, freq)
    high, mid, low = table_terms(np.concatenate([np.cos(inner), np.sin(inner)]) / ext)
    inverse_rows = [np.concatenate(p, axis=1) for p in ((high, high), (mid, mid), (low, high))]
    inverse_cols = [np.ascontiguousarray(part.T) for part in inverse_rows]
    unfold = np.zeros((tile, tile))
    for j in range(tile // 2):
        unfold[tile // 2 + j, j] = 1.0
        unfold[tile // 2 - 1 - j, tile // 2 + j] = 1.0
    unfold = unfold.astype(np.float32).astype(BF16)
    return (
        table_terms(forward_rows),
        table_terms(forward_cols),
        expand.astype(np.float32).astype(BF16),
        inverse_rows,
        inverse_cols,
        [unfold, np.ascontiguousarray(unfold.T)],
    )


def mm(a, b):
    return jnp.dot(a, b, preferred_element_type=F32)


def mm6(a, b):
    small = mm(a[2], b[0]) + mm(a[0], b[2]) + mm(a[1], b[1])
    return small + mm(a[1], b[0]) + mm(a[0], b[1]) + mm(a[0], b[0])


def strips_body(mask, rows, cols, length, orient, moves, corrected, current, send_a, send_b):
    tile = mask.shape[0]
    frags = rows.shape[2]
    first = lax.axis_index("ka") == 0
    even = lax.axis_index("tx") % 2 == 0
    place = lax.broadcasted_iota(jnp.int32, (tile, frags), 0)
    row_start = rows[0]
    col_start = cols[0]
    size = length[0]
    along_rows = orient[0] == 0
    state = mask[...]
    states = []
    for iteration in range(ITERS):
        shift = moves[0, 0, iteration : iteration + 1, :]
        lower = jnp.minimum(shift, 0)
        upper = jnp.maximum(shift, 0)
        row_low = jnp.where(along_rows, row_start, row_start + lower)
        row_high = jnp.where(along_rows, row_start + size, row_start + upper)
        col_low = jnp.where(along_rows, col_start + lower, col_start)
        col_high = jnp.where(along_rows, col_start + upper, col_start + size)
        sign = jnp.where(shift > 0, 1.0, jnp.where(shift < 0, -1.0, 0.0))
        in_rows = jnp.where((place >= row_low) & (place < row_high), sign, 0.0)
        in_cols = jnp.where((place >= col_low) & (place < col_high), 1.0, 0.0)
        strips = lax.dot_general(
            in_rows.astype(BF16),
            in_cols.astype(BF16),
            (((1,), (1,)), ((), ())),
            preferred_element_type=F32,
        )
        state = jnp.clip(state + strips, 0.0, 1.0)
        states.append(state)
    corrected[...] = states[1]
    mine = jnp.where(first, states[0], states[1])
    current[...] = mine
    top = mine[:HALO]
    bottom = mine[tile - HALO :]
    send_a[...] = jnp.where(even, bottom, top)
    send_b[...] = jnp.where(even, top, bottom)


def prepare_body(*refs, count):
    anchor, weights, weights_other, tolerance, site_rows, site_cols = refs[:6]
    tables_in = refs[6 : 6 + count]
    chosen, rows_out, scales, limits = refs[6 + count : 10 + count]
    tables_out = refs[10 + count : 10 + 2 * count]
    sems = refs[-1]
    copies = [
        pltpu.make_async_copy(source, target, sems.at[i])
        for i, (source, target) in enumerate(zip(tables_in, tables_out))
    ]
    for copy in copies:
        copy.start()
    which = lax.axis_index("ka")
    kernels = weights.shape[0]
    lanes = scales.shape[1]
    for k in range(kernels):
        scales[k : k + 1, :] = jnp.full((1, lanes), weights[k])
        scales[kernels + k : kernels + k + 1, :] = jnp.full((1, lanes), weights_other[k])
    limits[...] = jnp.full(limits.shape, tolerance[which].astype(F32) / 8.0)
    rows_out[...] = site_rows[...]
    place = lax.broadcasted_iota(jnp.int32, chosen.shape, 0)
    chosen[...] = jnp.where(place == site_cols[0], 1.0, 0.0).astype(BF16)
    for copy in copies:
        copy.wait()


def rows_body(current, got_a, got_b, high, mid, low, out, send_a, send_b):
    tile = current.shape[1]
    even = lax.axis_index("tx") % 2 == 0
    even_col = lax.axis_index("ty") % 2 == 0
    above = jnp.where(even, got_b[...], got_a[...])
    below = jnp.where(even, got_a[...], got_b[...])
    extended = jnp.concatenate([above, current[...], below], axis=0)
    result = mm6((high[...], mid[...], low[...]), terms(extended))
    out[...] = result
    left = result[:, :HALO]
    right = result[:, tile - HALO :]
    send_a[...] = jnp.where(even_col, right, left)
    send_b[...] = jnp.where(even_col, left, right)


def image_body(
    mine,
    got_a,
    got_b,
    spec_own,
    spec_other,
    scales,
    site_rows,
    chosen,
    limits,
    cols_high,
    cols_mid,
    cols_low,
    expand,
    inv_rows_a,
    inv_rows_b,
    inv_rows_c,
    inv_cols_a,
    inv_cols_b,
    inv_cols_c,
    unfold_rows,
    unfold_cols,
    pack,
    stats,
    image,
):
    tile = mine.shape[1]
    half = tile // 2
    even_col = lax.axis_index("ty") % 2 == 0
    left = jnp.where(even_col, got_b[...], got_a[...])
    right = jnp.where(even_col, got_a[...], got_b[...])
    window = jnp.concatenate([left, mine[...], right], axis=1)
    half_spec = terms(mm6(terms(window), (cols_high[...], cols_mid[...], cols_low[...])))
    quads = sum(mm(expand[...], part) for part in reversed(half_spec))
    spec_re = quads[:BAND, :BAND] + quads[BAND:, BAND:]
    spec_im = quads[BAND:, :BAND] - quads[:BAND, BAND:]
    count = spec_own.shape[0]
    sources = [(spec_own, k) for k in range(count)] + [(spec_other, k) for k in range(count)]
    for number, (spec, k) in enumerate(sources):
        kr = spec[k, 0]
        ki = spec[k, 1]
        product = jnp.concatenate(
            [kr * spec_re - ki * spec_im, kr * spec_im + ki * spec_re], axis=1
        )
        high, mid, low = terms(product)
        first = jnp.concatenate([high, mid], axis=0)
        second = jnp.concatenate([high, low], axis=0)
        inner = mm(inv_rows_c[...], second) + mm(inv_rows_b[...], first) + mm(inv_rows_a[...], first)
        even_re = inner[:half, :BAND]
        even_im = inner[:half, BAND:]
        odd_re = inner[half:, :BAND]
        odd_im = inner[half:, BAND:]
        folded = jnp.concatenate(
            [even_re - odd_im, even_re + odd_im, even_im + odd_re, even_im - odd_re], axis=0
        )
        high, mid, low = terms(folded)
        first = jnp.concatenate([high, mid], axis=1)
        second = jnp.concatenate([high, low], axis=1)
        field = mm(second, inv_cols_c[...]) + mm(first, inv_cols_b[...]) + mm(first, inv_cols_a[...])
        even_re = field[:tile, :half]
        odd_re = field[:tile, half:]
        even_im = field[tile:, :half]
        odd_im = field[tile:, half:]
        forth_re = even_re - odd_im
        forth_im = even_im + odd_re
        back_re = even_re + odd_im
        back_im = even_im - odd_re
        weight = scales[number : number + 1, :]
        forth = weight * (forth_re * forth_re + forth_im * forth_im)
        back = weight * (back_re * back_re + back_im * back_im)
        if number == 0:
            image[:, :half] = forth
            image[:, half:] = back
        else:
            image[:, :half] += forth
            image[:, half:] += back
    picture = sum(mm(unfold_rows[...], part) for part in reversed(terms(image[...])))
    picture = sum(mm(part, unfold_cols[...]) for part in reversed(terms(picture)))
    pack[:tile, :] = picture
    grad_rows = (pltpu.roll(picture, tile - 1, 0) - pltpu.roll(picture, 1, 0)) * 0.5
    grad_cols = (pltpu.roll(picture, tile - 1, 1) - pltpu.roll(picture, 1, 1)) * 0.5
    slope = jnp.sqrt(grad_rows * grad_rows + grad_cols * grad_cols)
    errors = terms((picture - LEVEL) / jnp.maximum(slope, SLOPE_FLOOR))
    sites = site_rows.shape[2]
    place = lax.broadcasted_iota(jnp.int32, (tile, tile), 0)
    limit = limits[...][0:1, 0:1]
    peak = None
    for j in range(sites // tile):
        lanes = slice(j * tile, (j + 1) * tile)
        sampled = mm(errors[0], chosen[:, lanes]) + mm(errors[1], chosen[:, lanes])
        found = jnp.sum(
            jnp.where(place == site_rows[0, :, lanes], sampled, 0.0), axis=0, keepdims=True
        )
        pack[tile + j : tile + j + 1, :] = found
        size = jnp.abs(found)
        share = 1.0 / (1.0 + jnp.exp(SHARPNESS * (size - limit)))
        if peak is None:
            peak, shares = size, share
        else:
            peak, shares = jnp.maximum(peak, size), shares + share
    lane = lax.broadcasted_iota(jnp.int32, stats.shape, 1)
    stats[...] = jnp.where(lane == 0, jnp.max(peak), jnp.sum(shares))


def final_body(pack, other, stats, intensity, errors, peaks, shares, *, total):
    tile = pack.shape[1]
    first = lax.axis_index("ka") == 0
    intensity[...] = jnp.where(first, other[:tile, :], pack[:tile, :])
    mine = pack[tile:, :]
    theirs = other[tile:, :]
    zero = jnp.where(first, mine, theirs)
    one = jnp.where(first, theirs, mine)
    for j in range(errors.shape[3] // tile):
        lanes = slice(j * tile, (j + 1) * tile)
        errors[0, 0, 0:1, lanes] = zero[j : j + 1]
        errors[0, 0, 1:2, lanes] = one[j : j + 1]
    got = stats[...]
    iteration = lax.broadcasted_iota(jnp.int32, got.shape, 0) % ITERS
    lane = lax.broadcasted_iota(jnp.int32, got.shape, 1)
    for t in range(ITERS):
        peaks[t] = jnp.max(jnp.where((iteration == t) & (lane == 0), got, 0.0))
        shares[t] = jnp.sum(jnp.where((iteration == t) & (lane == 1), got, 0.0)) / total


def spec(count, space=VMEM):
    return [pl.BlockSpec(memory_space=space)] * count


def in_hbm(x):
    return pltpu.with_memory_space_constraint(x, pltpu.MemorySpace.HBM)


def shape(*dims):
    return jax.ShapeDtypeStruct(dims, F32)


def neighbours(axis, send_a, send_b):
    count = lax.axis_size(axis)
    got = []
    for start, sent in ((0, send_a), (1, send_b)):
        pairs = [(i, i + 1) for i in range(start, count - 1, 2)]
        if pairs:
            got.append(lax.ppermute(sent, axis, pairs + [(b, a) for a, b in pairs]))
        else:
            got.append(jnp.zeros_like(sent))
    return got


def shards(
    mask_raster,
    frag_rows,
    frag_cols,
    frag_length,
    frag_orient,
    frag_moves,
    site_rows,
    site_cols,
    spectra,
    weights,
    tolerance,
):
    tile = mask_raster.shape[0]
    sites = site_rows.shape[2]
    fwd_rows, fwd_cols, expand, inv_rows, inv_cols, unfold = tables(tile)
    half_rows = fwd_rows[0].shape[0]
    swap = [(0, 1), (1, 0)]
    spectra_other = lax.ppermute(spectra, "ka", swap)
    weights_other = lax.ppermute(weights, "ka", swap)
    corrected, current, send_a, send_b = pl.pallas_call(
        strips_body,
        out_shape=[shape(tile, tile), shape(tile, tile), shape(HALO, tile), shape(HALO, tile)],
        in_specs=spec(6),
        out_specs=spec(4),
        compiler_params=LIMIT,
        name="strips",
    )(*map(in_hbm, (mask_raster, frag_rows, frag_cols, frag_length, frag_orient, frag_moves)))
    got_a, got_b = neighbours("tx", send_a, send_b)
    constants = [*fwd_rows, *fwd_cols, expand, *inv_rows, *inv_cols, *unfold]
    members = lax.axis_size("tx") * lax.axis_size("ty") * lax.axis_size("ka")
    kernels = spectra.shape[0] * lax.axis_size("ka")
    chosen, rows_at, scales, limits, *constants = pl.pallas_call(
        functools.partial(prepare_body, count=len(constants)),
        out_shape=[
            jax.ShapeDtypeStruct((tile, sites), BF16),
            jax.ShapeDtypeStruct(site_rows.shape, jnp.int32),
            shape(kernels, 128),
            shape(8, 128),
        ]
        + [jax.ShapeDtypeStruct(c.shape, BF16) for c in constants],
        in_specs=spec(1, pl.ANY) + spec(3, SMEM) + spec(2) + spec(len(constants), pl.ANY),
        out_specs=spec(4 + len(constants)),
        scratch_shapes=[pltpu.SemaphoreType.DMA((len(constants),))],
        compiler_params=LIMIT,
        name="prepare",
    )(
        send_a,
        weights,
        weights_other,
        tolerance,
        in_hbm(site_rows),
        in_hbm(site_cols),
        *[in_hbm(jnp.asarray(c)) for c in constants],
    )
    mine, send_a, send_b = pl.pallas_call(
        rows_body,
        out_shape=[shape(half_rows, tile), shape(half_rows, HALO), shape(half_rows, HALO)],
        in_specs=spec(6),
        out_specs=spec(3),
        compiler_params=LIMIT,
        name="rows",
    )(current, got_a, got_b, *constants[:3])
    got_a, got_b = neighbours("ty", send_a, send_b)
    pack_rows = tile + sites // tile
    pack, stats = pl.pallas_call(
        image_body,
        out_shape=[shape(pack_rows, tile), shape(members, 128)],
        in_specs=spec(9 + len(constants) - 3),
        out_specs=spec(2),
        scratch_shapes=[pltpu.VMEM((tile, tile), F32)],
        compiler_params=LIMIT,
        name="image",
    )(
        mine,
        got_a,
        got_b,
        spectra,
        spectra_other,
        scales,
        rows_at,
        chosen,
        limits,
        *constants[3:],
    )
    other = lax.ppermute(pack, "ka", swap)
    merged = lax.all_to_all(stats, ("tx", "ty", "ka"), 0, 0, tiled=True)
    total = float(sites * lax.axis_size("tx") * lax.axis_size("ty"))
    intensity, errors, peaks, shares = pl.pallas_call(
        functools.partial(final_body, total=total),
        out_shape=[shape(tile, tile), shape(1, 1, ITERS, sites), shape(ITERS), shape(ITERS)],
        in_specs=spec(3),
        out_specs=spec(2) + spec(2, SMEM),
        compiler_params=LIMIT,
        name="final",
    )(pack, other, merged)
    return (intensity, corrected, errors, peaks, shares)


def solution(mesh):
    assert mesh.shape["ka"] == ITERS
    placed = (
        P(("groups", "tx"), "ty"),
        P(("groups", "tx"), "ty", None),
        P(("groups", "tx"), "ty", None),
        P(("groups", "tx"), "ty", None),
        P(("groups", "tx"), "ty", None),
        P(("groups", "tx"), "ty", None, None),
        P(("groups", "tx"), "ty", None),
        P(("groups", "tx"), "ty", None),
        P("ka", None, None, None),
        P("ka"),
        P(),
    )
    return jax.shard_map(
        shards,
        mesh=mesh,
        in_specs=placed,
        out_specs=(
            P(("groups", "tx"), "ty"),
            P(("groups", "tx"), "ty"),
            P(("groups", "tx"), "ty", None, None),
            P("groups"),
            P("groups"),
        ),
        check_vma=False,
    )
```

```python
import functools
import math

import jax
import jax.numpy as jnp
import numpy as np
from jax import lax
from jax.experimental import pallas as pl
from jax.experimental.pallas import tpu as pltpu
from jax.sharding import PartitionSpec as P


HALO = 128
BAND = 128
ITERS = 2

LEVEL = 0.4
SLOPE_FLOOR = 0.05
SHARPNESS = 8.0

F32 = jnp.float32
BF16 = jnp.bfloat16
VMEM = pltpu.MemorySpace.VMEM
SMEM = pltpu.MemorySpace.SMEM
PAD_ROWS = 16
LIMIT = pltpu.CompilerParams(vmem_limit_bytes=24 * 1024 * 1024)


def terms(x):
    high = x.astype(BF16)
    rest = x - high.astype(F32)
    mid = rest.astype(BF16)
    return high, mid, (rest - mid.astype(F32)).astype(BF16)


def table_terms(table):
    out = []
    for _ in range(3):
        part = table.astype(np.float32).astype(BF16)
        out.append(part)
        table = table - part.astype(np.float64)
    return out


@functools.lru_cache(maxsize=None)
def tables(tile):
    ext = tile + 2 * HALO
    half = BAND // 2
    rows = (BAND + 1 + PAD_ROWS - 1) // PAD_ROWS * PAD_ROWS
    step = 2.0 * math.pi / ext
    place = np.arange(ext) - (ext - 1) / 2
    freq = np.arange(BAND) - half

    def angle(freqs, places):
        return freqs[:, None] * places[None, :] * step

    forward_rows = np.zeros((rows, ext))
    forward_rows[: half + 1] = np.cos(angle(np.arange(half + 1), place))
    forward_rows[half + 1 : BAND + 1] = -np.sin(angle(np.arange(1, half + 1), place))
    turn = angle(place, freq)
    forward_cols = np.concatenate([np.cos(turn), np.sin(turn)], axis=1)
    expand = np.zeros((2 * BAND, rows))
    for index, f in enumerate(freq):
        expand[index, abs(f)] = 1.0
        if f != 0:
            expand[BAND + index, half + abs(f)] = np.sign(f)
    inner = angle(np.arange(tile // 2) + 0.5, freq)
    high, mid, low = table_terms(np.concatenate([np.cos(inner), np.sin(inner)]) / ext)
    inverse_rows = [np.concatenate(p, axis=1) for p in ((high, high), (mid, mid), (low, high))]
    inverse_cols = [np.ascontiguousarray(part.T) for part in inverse_rows]
    unfold = np.zeros((tile, tile))
    for j in range(tile // 2):
        unfold[tile // 2 + j, j] = 1.0
        unfold[tile // 2 - 1 - j, tile // 2 + j] = 1.0
    unfold = unfold.astype(np.float32).astype(BF16)
    return (
        table_terms(forward_rows),
        table_terms(forward_cols),
        expand.astype(np.float32).astype(BF16),
        inverse_rows,
        inverse_cols,
        [unfold, np.ascontiguousarray(unfold.T)],
    )


def mm(a, b):
    return jnp.dot(a, b, preferred_element_type=F32)


def mm6(a, b):
    small = mm(a[2], b[0]) + mm(a[0], b[2]) + mm(a[1], b[1])
    return small + mm(a[1], b[0]) + mm(a[0], b[1]) + mm(a[0], b[0])


def strips_body(mask, rows, cols, length, orient, moves, corrected, current, send_a, send_b):
    tile = mask.shape[0]
    frags = rows.shape[2]
    first = lax.axis_index("ka") == 0
    even = lax.axis_index("tx") % 2 == 0
    place = lax.broadcasted_iota(jnp.int32, (tile, frags), 0)
    row_start = rows[0]
    col_start = cols[0]
    size = length[0]
    along_rows = orient[0] == 0
    state = mask[...]
    states = []
    for iteration in range(ITERS):
        shift = moves[0, 0, iteration : iteration + 1, :]
        lower = jnp.minimum(shift, 0)
        upper = jnp.maximum(shift, 0)
        row_low = jnp.where(along_rows, row_start, row_start + lower)
        row_high = jnp.where(along_rows, row_start + size, row_start + upper)
        col_low = jnp.where(along_rows, col_start + lower, col_start)
        col_high = jnp.where(along_rows, col_start + upper, col_start + size)
        sign = jnp.where(shift > 0, 1.0, jnp.where(shift < 0, -1.0, 0.0))
        in_rows = jnp.where((place >= row_low) & (place < row_high), sign, 0.0)
        in_cols = jnp.where((place >= col_low) & (place < col_high), 1.0, 0.0)
        strips = lax.dot_general(
            in_rows.astype(BF16),
            in_cols.astype(BF16),
            (((1,), (1,)), ((), ())),
            preferred_element_type=F32,
        )
        state = jnp.clip(state + strips, 0.0, 1.0)
        states.append(state)
    corrected[...] = states[1]
    mine = jnp.where(first, states[0], states[1])
    current[...] = mine
    top = mine[:HALO]
    bottom = mine[tile - HALO :]
    send_a[...] = jnp.where(even, bottom, top)
    send_b[...] = jnp.where(even, top, bottom)


def prepare_rows_body(anchor, weights, spectra, *refs, count):
    tables_in = refs[:count]
    scaled = refs[count]
    tables_out = refs[count + 1 : 2 * count + 1]
    sems = refs[-1]
    copies = [
        pltpu.make_async_copy(source, target, sems.at[i])
        for i, (source, target) in enumerate(zip([spectra, *tables_in], [scaled, *tables_out]))
    ]
    for copy in copies:
        copy.start()
    copies[0].wait()
    lanes = scaled.shape[3]
    for k in range(scaled.shape[0]):
        factor = jnp.sqrt(jnp.full((1, 1, lanes), weights[k]))
        scaled[k] = scaled[k] * factor
    for copy in copies[1:]:
        copy.wait()


def prepare_image_body(*refs, count):
    _, tolerance, site_rows, site_cols = refs[:4]
    tables_in = refs[4 : 4 + count]
    chosen, rows_out, limits = refs[4 + count : 7 + count]
    tables_out = refs[7 + count : 7 + 2 * count]
    sems = refs[-1]
    copies = [
        pltpu.make_async_copy(source, target, sems.at[i])
        for i, (source, target) in enumerate(zip(tables_in, tables_out))
    ]
    for copy in copies:
        copy.start()
    which = lax.axis_index("ka")
    limits[...] = jnp.full(limits.shape, tolerance[which].astype(F32) / 8.0)
    rows_out[...] = site_rows[...]
    place = lax.broadcasted_iota(jnp.int32, chosen.shape, 0)
    chosen[...] = jnp.where(place == site_cols[0], 1.0, 0.0).astype(BF16)
    for copy in copies:
        copy.wait()


def rows_body(current, got_a, got_b, high, mid, low, out, send_a, send_b):
    tile = current.shape[1]
    even = lax.axis_index("tx") % 2 == 0
    even_col = lax.axis_index("ty") % 2 == 0
    above = jnp.where(even, got_b[...], got_a[...])
    below = jnp.where(even, got_a[...], got_b[...])
    extended = jnp.concatenate([above, current[...], below], axis=0)
    result = mm6((high[...], mid[...], low[...]), terms(extended))
    out[...] = result
    left = result[:, :HALO]
    right = result[:, tile - HALO :]
    send_a[...] = jnp.where(even_col, right, left)
    send_b[...] = jnp.where(even_col, left, right)


def image_body(
    mine,
    got_a,
    got_b,
    spec_own,
    spec_other,
    site_rows,
    chosen,
    limits,
    cols_high,
    cols_mid,
    cols_low,
    expand,
    inv_rows_a,
    inv_rows_b,
    inv_rows_c,
    inv_cols_a,
    inv_cols_b,
    inv_cols_c,
    unfold_rows,
    unfold_cols,
    pack,
    stats,
    image,
):
    tile = mine.shape[1]
    half = tile // 2
    even_col = lax.axis_index("ty") % 2 == 0
    left = jnp.where(even_col, got_b[...], got_a[...])
    right = jnp.where(even_col, got_a[...], got_b[...])
    window = jnp.concatenate([left, mine[...], right], axis=1)
    half_spec = terms(mm6(terms(window), (cols_high[...], cols_mid[...], cols_low[...])))
    quads = sum(mm(expand[...], part) for part in reversed(half_spec))
    spec_re = quads[:BAND, :BAND] + quads[BAND:, BAND:]
    spec_im = quads[BAND:, :BAND] - quads[:BAND, BAND:]
    count = spec_own.shape[0]
    sources = [(spec_own, k) for k in range(count)] + [(spec_other, k) for k in range(count)]
    for number, (spec, k) in enumerate(sources):
        kr = spec[k, 0]
        ki = spec[k, 1]
        product = jnp.concatenate(
            [kr * spec_re - ki * spec_im, kr * spec_im + ki * spec_re], axis=1
        )
        high, mid, low = terms(product)
        first = jnp.concatenate([high, mid], axis=0)
        second = jnp.concatenate([high, low], axis=0)
        inner = mm(inv_rows_c[...], second) + mm(inv_rows_b[...], first) + mm(inv_rows_a[...], first)
        even_re = inner[:half, :BAND]
        even_im = inner[:half, BAND:]
        odd_re = inner[half:, :BAND]
        odd_im = inner[half:, BAND:]
        folded = jnp.concatenate(
            [even_re - odd_im, even_re + odd_im, even_im + odd_re, even_im - odd_re], axis=0
        )
        high, mid, low = terms(folded)
        first = jnp.concatenate([high, mid], axis=1)
        second = jnp.concatenate([high, low], axis=1)
        field = mm(second, inv_cols_c[...]) + mm(first, inv_cols_b[...]) + mm(first, inv_cols_a[...])
        even_re = field[:tile, :half]
        odd_re = field[:tile, half:]
        even_im = field[tile:, :half]
        odd_im = field[tile:, half:]
        forth_re = even_re - odd_im
        forth_im = even_im + odd_re
        back_re = even_re + odd_im
        back_im = even_im - odd_re
        forth = forth_re * forth_re + forth_im * forth_im
        back = back_re * back_re + back_im * back_im
        if number == 0:
            image[:, :half] = forth
            image[:, half:] = back
        else:
            image[:, :half] += forth
            image[:, half:] += back
    picture = sum(mm(unfold_rows[...], part) for part in reversed(terms(image[...])))
    picture = sum(mm(part, unfold_cols[...]) for part in reversed(terms(picture)))
    pack[:tile, :] = picture
    grad_rows = (pltpu.roll(picture, tile - 1, 0) - pltpu.roll(picture, 1, 0)) * 0.5
    grad_cols = (pltpu.roll(picture, tile - 1, 1) - pltpu.roll(picture, 1, 1)) * 0.5
    slope = jnp.sqrt(grad_rows * grad_rows + grad_cols * grad_cols)
    errors = terms((picture - LEVEL) / jnp.maximum(slope, SLOPE_FLOOR))
    sites = site_rows.shape[2]
    place = lax.broadcasted_iota(jnp.int32, (tile, tile), 0)
    limit = limits[...][0:1, 0:1]
    peak = None
    for j in range(sites // tile):
        lanes = slice(j * tile, (j + 1) * tile)
        sampled = mm(errors[0], chosen[:, lanes]) + mm(errors[1], chosen[:, lanes])
        found = jnp.sum(
            jnp.where(place == site_rows[0, :, lanes], sampled, 0.0), axis=0, keepdims=True
        )
        pack[tile + j : tile + j + 1, :] = found
        size = jnp.abs(found)
        share = 1.0 / (1.0 + jnp.exp(SHARPNESS * (size - limit)))
        if peak is None:
            peak, shares = size, share
        else:
            peak, shares = jnp.maximum(peak, size), shares + share
    lane = lax.broadcasted_iota(jnp.int32, stats.shape, 1)
    stats[...] = jnp.where(lane == 0, jnp.max(peak), jnp.sum(shares))


def final_body(pack, other, stats, intensity, errors, peaks, shares, *, total):
    tile = pack.shape[1]
    first = lax.axis_index("ka") == 0
    intensity[...] = jnp.where(first, other[:tile, :], pack[:tile, :])
    mine = pack[tile:, :]
    theirs = other[tile:, :]
    zero = jnp.where(first, mine, theirs)
    one = jnp.where(first, theirs, mine)
    for j in range(errors.shape[3] // tile):
        lanes = slice(j * tile, (j + 1) * tile)
        errors[0, 0, 0:1, lanes] = zero[j : j + 1]
        errors[0, 0, 1:2, lanes] = one[j : j + 1]
    got = stats[...]
    iteration = lax.broadcasted_iota(jnp.int32, got.shape, 0) % ITERS
    lane = lax.broadcasted_iota(jnp.int32, got.shape, 1)
    for t in range(ITERS):
        peaks[t] = jnp.max(jnp.where((iteration == t) & (lane == 0), got, 0.0))
        shares[t] = jnp.sum(jnp.where((iteration == t) & (lane == 1), got, 0.0)) / total


def spec(count, space=VMEM):
    return [pl.BlockSpec(memory_space=space)] * count


def in_hbm(x):
    return pltpu.with_memory_space_constraint(x, pltpu.MemorySpace.HBM)


def shape(*dims):
    return jax.ShapeDtypeStruct(dims, F32)


def neighbours(axis, send_a, send_b):
    count = lax.axis_size(axis)
    got = []
    for start, sent in ((0, send_a), (1, send_b)):
        pairs = [(i, i + 1) for i in range(start, count - 1, 2)]
        if pairs:
            got.append(lax.ppermute(sent, axis, pairs + [(b, a) for a, b in pairs]))
        else:
            got.append(jnp.zeros_like(sent))
    return got


def shards(
    mask_raster,
    frag_rows,
    frag_cols,
    frag_length,
    frag_orient,
    frag_moves,
    site_rows,
    site_cols,
    spectra,
    weights,
    tolerance,
):
    tile = mask_raster.shape[0]
    sites = site_rows.shape[2]
    fwd_rows, fwd_cols, expand, inv_rows, inv_cols, unfold = tables(tile)
    half_rows = fwd_rows[0].shape[0]
    swap = [(0, 1), (1, 0)]
    corrected, current, send_a, send_b = pl.pallas_call(
        strips_body,
        out_shape=[shape(tile, tile), shape(tile, tile), shape(HALO, tile), shape(HALO, tile)],
        in_specs=spec(6),
        out_specs=spec(4),
        compiler_params=LIMIT,
        name="strips",
    )(*map(in_hbm, (mask_raster, frag_rows, frag_cols, frag_length, frag_orient, frag_moves)))
    got_a, got_b = neighbours("tx", send_a, send_b)
    scaled, *row_tables = pl.pallas_call(
        functools.partial(prepare_rows_body, count=len(fwd_rows)),
        out_shape=[shape(*spectra.shape)]
        + [jax.ShapeDtypeStruct(c.shape, BF16) for c in fwd_rows],
        in_specs=spec(1, pl.ANY) + spec(1, SMEM) + spec(1 + len(fwd_rows), pl.ANY),
        out_specs=spec(1 + len(fwd_rows)),
        scratch_shapes=[pltpu.SemaphoreType.DMA((1 + len(fwd_rows),))],
        compiler_params=LIMIT,
        name="prepare_rows",
    )(send_a, weights, in_hbm(spectra), *[in_hbm(jnp.asarray(c)) for c in fwd_rows])
    scaled_other = lax.ppermute(scaled, "ka", swap)
    mine, send_a, send_b = pl.pallas_call(
        rows_body,
        out_shape=[shape(half_rows, tile), shape(half_rows, HALO), shape(half_rows, HALO)],
        in_specs=spec(6),
        out_specs=spec(3),
        compiler_params=LIMIT,
        name="rows",
    )(current, got_a, got_b, *row_tables)
    got_a, got_b = neighbours("ty", send_a, send_b)
    constants = [*fwd_cols, expand, *inv_rows, *inv_cols, *unfold]
    chosen, rows_at, limits, *constants = pl.pallas_call(
        functools.partial(prepare_image_body, count=len(constants)),
        out_shape=[
            jax.ShapeDtypeStruct((tile, sites), BF16),
            jax.ShapeDtypeStruct(site_rows.shape, jnp.int32),
            shape(8, 128),
        ]
        + [jax.ShapeDtypeStruct(c.shape, BF16) for c in constants],
        in_specs=spec(1, pl.ANY) + spec(1, SMEM) + spec(2) + spec(len(constants), pl.ANY),
        out_specs=spec(3 + len(constants)),
        scratch_shapes=[pltpu.SemaphoreType.DMA((len(constants),))],
        compiler_params=LIMIT,
        name="prepare_image",
    )(
        send_a,
        tolerance,
        in_hbm(site_rows),
        in_hbm(site_cols),
        *[in_hbm(jnp.asarray(c)) for c in constants],
    )
    members = lax.axis_size("tx") * lax.axis_size("ty") * lax.axis_size("ka")
    pack_rows = tile + sites // tile
    pack, stats = pl.pallas_call(
        image_body,
        out_shape=[shape(pack_rows, tile), shape(members, 128)],
        in_specs=spec(8 + len(constants)),
        out_specs=spec(2),
        scratch_shapes=[pltpu.VMEM((tile, tile), F32)],
        compiler_params=LIMIT,
        name="image",
    )(
        mine,
        got_a,
        got_b,
        scaled,
        scaled_other,
        rows_at,
        chosen,
        limits,
        *constants,
    )
    other = lax.ppermute(pack, "ka", swap)
    merged = lax.all_to_all(stats, ("tx", "ty", "ka"), 0, 0, tiled=True)
    total = float(sites * lax.axis_size("tx") * lax.axis_size("ty"))
    intensity, errors, peaks, shares = pl.pallas_call(
        functools.partial(final_body, total=total),
        out_shape=[shape(tile, tile), shape(1, 1, ITERS, sites), shape(ITERS), shape(ITERS)],
        in_specs=spec(3),
        out_specs=spec(2) + spec(2, SMEM),
        compiler_params=LIMIT,
        name="final",
    )(pack, other, merged)
    return (intensity, corrected, errors, peaks, shares)


def solution(mesh):
    assert mesh.shape["ka"] == ITERS
    placed = (
        P(("groups", "tx"), "ty"),
        P(("groups", "tx"), "ty", None),
        P(("groups", "tx"), "ty", None),
        P(("groups", "tx"), "ty", None),
        P(("groups", "tx"), "ty", None),
        P(("groups", "tx"), "ty", None, None),
        P(("groups", "tx"), "ty", None),
        P(("groups", "tx"), "ty", None),
        P("ka", None, None, None),
        P("ka"),
        P(),
    )
    return jax.shard_map(
        shards,
        mesh=mesh,
        in_specs=placed,
        out_specs=(
            P(("groups", "tx"), "ty"),
            P(("groups", "tx"), "ty"),
            P(("groups", "tx"), "ty", None, None),
            P("groups"),
            P("groups"),
        ),
        check_vma=False,
    )
```

```python
import functools
import math

import jax
import jax.numpy as jnp
import numpy as np
from jax import lax
from jax.experimental import pallas as pl
from jax.experimental.pallas import tpu as pltpu
from jax.sharding import PartitionSpec as P


HALO = 128
BAND = 128
ITERS = 2

LEVEL = 0.4
SLOPE_FLOOR = 0.05
SHARPNESS = 8.0

F32 = jnp.float32
BF16 = jnp.bfloat16
VMEM = pltpu.MemorySpace.VMEM
SMEM = pltpu.MemorySpace.SMEM
PAD_ROWS = 16
LIMIT = pltpu.CompilerParams(vmem_limit_bytes=24 * 1024 * 1024)


def terms(x):
    high = x.astype(BF16)
    rest = x - high.astype(F32)
    mid = rest.astype(BF16)
    return high, mid, (rest - mid.astype(F32)).astype(BF16)


def table_terms(table):
    out = []
    for _ in range(3):
        part = table.astype(np.float32).astype(BF16)
        out.append(part)
        table = table - part.astype(np.float64)
    return out


@functools.lru_cache(maxsize=None)
def tables(tile):
    ext = tile + 2 * HALO
    half = BAND // 2
    rows = (BAND + 1 + PAD_ROWS - 1) // PAD_ROWS * PAD_ROWS
    step = 2.0 * math.pi / ext
    place = np.arange(ext) - (ext - 1) / 2
    freq = np.arange(BAND) - half

    def angle(freqs, places):
        return freqs[:, None] * places[None, :] * step

    forward_rows = np.zeros((rows, ext))
    forward_rows[: half + 1] = np.cos(angle(np.arange(half + 1), place))
    forward_rows[half + 1 : BAND + 1] = -np.sin(angle(np.arange(1, half + 1), place))
    turn = angle(place, freq)
    forward_cols = np.concatenate([np.cos(turn), np.sin(turn)], axis=1)
    expand = np.zeros((2 * BAND, rows))
    for index, f in enumerate(freq):
        expand[index, abs(f)] = 1.0
        if f != 0:
            expand[BAND + index, half + abs(f)] = np.sign(f)
    inner = angle(np.arange(tile // 2) + 0.5, freq)
    high, mid, low = table_terms(np.concatenate([np.cos(inner), np.sin(inner)]) / ext)
    inverse_rows = [np.concatenate(p, axis=1) for p in ((high, high), (mid, mid), (low, high))]
    inverse_cols = [np.ascontiguousarray(part.T) for part in inverse_rows]
    unfold = np.zeros((tile, tile))
    for j in range(tile // 2):
        unfold[tile // 2 + j, j] = 1.0
        unfold[tile // 2 - 1 - j, tile // 2 + j] = 1.0
    unfold = unfold.astype(np.float32).astype(BF16)
    return (
        table_terms(forward_rows),
        table_terms(forward_cols),
        expand.astype(np.float32).astype(BF16),
        inverse_rows,
        inverse_cols,
        [unfold, np.ascontiguousarray(unfold.T)],
    )


def mm(a, b):
    return jnp.dot(a, b, preferred_element_type=F32)


def mm6(a, b):
    small = mm(a[2], b[0]) + mm(a[0], b[2]) + mm(a[1], b[1])
    return small + mm(a[1], b[0]) + mm(a[0], b[1]) + mm(a[0], b[0])


def strips_body(mask, rows, cols, length, orient, moves, corrected, current, send_a, send_b):
    tile = mask.shape[0]
    frags = rows.shape[2]
    first = lax.axis_index("ka") == 0
    even = lax.axis_index("tx") % 2 == 0
    place = lax.broadcasted_iota(jnp.int32, (tile, frags), 0)
    row_start = rows[0]
    col_start = cols[0]
    size = length[0]
    along_rows = orient[0] == 0
    state = mask[...]
    states = []
    for iteration in range(ITERS):
        shift = moves[0, 0, iteration : iteration + 1, :]
        lower = jnp.minimum(shift, 0)
        upper = jnp.maximum(shift, 0)
        row_low = jnp.where(along_rows, row_start, row_start + lower)
        row_high = jnp.where(along_rows, row_start + size, row_start + upper)
        col_low = jnp.where(along_rows, col_start + lower, col_start)
        col_high = jnp.where(along_rows, col_start + upper, col_start + size)
        sign = jnp.where(shift > 0, 1.0, jnp.where(shift < 0, -1.0, 0.0))
        in_rows = jnp.where((place >= row_low) & (place < row_high), sign, 0.0)
        in_cols = jnp.where((place >= col_low) & (place < col_high), 1.0, 0.0)
        strips = lax.dot_general(
            in_rows.astype(BF16),
            in_cols.astype(BF16),
            (((1,), (1,)), ((), ())),
            preferred_element_type=F32,
        )
        state = jnp.clip(state + strips, 0.0, 1.0)
        states.append(state)
    corrected[...] = states[1]
    mine = jnp.where(first, states[0], states[1])
    current[...] = mine
    top = mine[:HALO]
    bottom = mine[tile - HALO :]
    send_a[...] = jnp.where(even, bottom, top)
    send_b[...] = jnp.where(even, top, bottom)


def prepare_rows_body(anchor, weights, spectra, *refs, count):
    tables_in = refs[:count]
    scaled = refs[count]
    tables_out = refs[count + 1 : 2 * count + 1]
    sems = refs[-1]
    copies = [
        pltpu.make_async_copy(source, target, sems.at[i])
        for i, (source, target) in enumerate(zip([spectra, *tables_in], [scaled, *tables_out]))
    ]
    for copy in copies:
        copy.start()
    copies[0].wait()
    lanes = scaled.shape[3]
    for k in range(scaled.shape[0]):
        factor = jnp.sqrt(jnp.full((1, 1, lanes), weights[k]))
        scaled[k] = scaled[k] * factor
    for copy in copies[1:]:
        copy.wait()


def prepare_image_body(*refs, count):
    _, tolerance, site_rows, site_cols = refs[:4]
    tables_in = refs[4 : 4 + count]
    chosen, rows_out, limits = refs[4 + count : 7 + count]
    tables_out = refs[7 + count : 7 + 2 * count]
    sems = refs[-1]
    copies = [
        pltpu.make_async_copy(source, target, sems.at[i])
        for i, (source, target) in enumerate(zip(tables_in, tables_out))
    ]
    for copy in copies:
        copy.start()
    which = lax.axis_index("ka")
    limits[...] = jnp.full(limits.shape, tolerance[which].astype(F32) / 8.0)
    tile = chosen.shape[0]

    def folded(position):
        return jnp.where(position >= tile // 2, position - tile // 2, tile - 1 - position)

    rows_out[...] = folded(site_rows[...])
    place = lax.broadcasted_iota(jnp.int32, chosen.shape, 0)
    chosen[...] = jnp.where(place == folded(site_cols[0]), 1.0, 0.0).astype(BF16)
    for copy in copies:
        copy.wait()


def rows_body(current, got_a, got_b, high, mid, low, out, send_a, send_b):
    tile = current.shape[1]
    even = lax.axis_index("tx") % 2 == 0
    even_col = lax.axis_index("ty") % 2 == 0
    above = jnp.where(even, got_b[...], got_a[...])
    below = jnp.where(even, got_a[...], got_b[...])
    extended = jnp.concatenate([above, current[...], below], axis=0)
    result = mm6((high[...], mid[...], low[...]), terms(extended))
    out[...] = result
    left = result[:, :HALO]
    right = result[:, tile - HALO :]
    send_a[...] = jnp.where(even_col, right, left)
    send_b[...] = jnp.where(even_col, left, right)


def fold_difference(x, axis):
    half = x.shape[axis] // 2
    sides = (lax.slice_in_dim(x, 0, half, axis=axis), lax.slice_in_dim(x, half, 2 * half, axis=axis))
    out = []
    for side, other in (sides, sides[::-1]):
        first = lax.broadcasted_iota(jnp.int32, side.shape, axis) == 0
        edge = lax.slice_in_dim(other, 0, 1, axis=axis)
        inward = jnp.where(first, edge, pltpu.roll(side, 1, axis))
        out.append(pltpu.roll(side, half - 1, axis) - inward)
    return jnp.concatenate(out, axis=axis)


def image_body(
    mine,
    got_a,
    got_b,
    spec_own,
    spec_other,
    site_rows,
    chosen,
    limits,
    cols_high,
    cols_mid,
    cols_low,
    expand,
    inv_rows_a,
    inv_rows_b,
    inv_rows_c,
    inv_cols_a,
    inv_cols_b,
    inv_cols_c,
    unfold_rows,
    unfold_cols,
    pack,
    stats,
    image,
):
    tile = mine.shape[1]
    half = tile // 2
    even_col = lax.axis_index("ty") % 2 == 0
    left = jnp.where(even_col, got_b[...], got_a[...])
    right = jnp.where(even_col, got_a[...], got_b[...])
    window = jnp.concatenate([left, mine[...], right], axis=1)
    half_spec = terms(mm6(terms(window), (cols_high[...], cols_mid[...], cols_low[...])))
    quads = sum(mm(expand[...], part) for part in reversed(half_spec))
    spec_re = quads[:BAND, :BAND] + quads[BAND:, BAND:]
    spec_im = quads[BAND:, :BAND] - quads[:BAND, BAND:]
    count = spec_own.shape[0]
    image[...] = jnp.zeros(image.shape, F32)

    def add_kernel(spec, k):
        kr = spec[k, 0]
        ki = spec[k, 1]
        product = jnp.concatenate(
            [kr * spec_re - ki * spec_im, kr * spec_im + ki * spec_re], axis=1
        )
        high, mid, low = terms(product)
        first = jnp.concatenate([high, mid], axis=0)
        second = jnp.concatenate([high, low], axis=0)
        inner = mm(inv_rows_c[...], second) + mm(inv_rows_b[...], first) + mm(inv_rows_a[...], first)
        even_re = inner[:half, :BAND]
        even_im = inner[:half, BAND:]
        odd_re = inner[half:, :BAND]
        odd_im = inner[half:, BAND:]
        folded = jnp.concatenate(
            [even_re - odd_im, even_re + odd_im, even_im + odd_re, even_im - odd_re], axis=0
        )
        high, mid, low = terms(folded)
        first = jnp.concatenate([high, mid], axis=1)
        second = jnp.concatenate([high, low], axis=1)
        field = mm(second, inv_cols_c[...]) + mm(first, inv_cols_b[...]) + mm(first, inv_cols_a[...])
        even_re = field[:tile, :half]
        odd_re = field[:tile, half:]
        even_im = field[tile:, :half]
        odd_im = field[tile:, half:]
        forth_re = even_re - odd_im
        forth_im = even_im + odd_re
        back_re = even_re + odd_im
        back_im = even_im - odd_re
        forth = forth_re * forth_re + forth_im * forth_im
        back = back_re * back_re + back_im * back_im
        image[:, :half] += forth
        image[:, half:] += back

    def add_kernels(step, carry):
        for j in range(4):
            add_kernel(spec_own, step * 4 + j)
            add_kernel(spec_other, step * 4 + j)
        return carry

    lax.fori_loop(0, count // 4, add_kernels, 0)
    picture = image[...]
    grad_rows = fold_difference(picture, 0) * 0.5
    grad_cols = fold_difference(picture, 1) * 0.5
    slope = jnp.sqrt(grad_rows * grad_rows + grad_cols * grad_cols)
    errors = terms((picture - LEVEL) / jnp.maximum(slope, SLOPE_FLOOR))
    sites = site_rows.shape[2]
    place = lax.broadcasted_iota(jnp.int32, (tile, tile), 0)
    limit = limits[...][0:1, 0:1]
    peak = None
    for j in range(sites // tile):
        lanes = slice(j * tile, (j + 1) * tile)
        sampled = mm(errors[0], chosen[:, lanes]) + mm(errors[1], chosen[:, lanes])
        found = jnp.sum(
            jnp.where(place == site_rows[0, :, lanes], sampled, 0.0), axis=0, keepdims=True
        )
        pack[tile + j : tile + j + 1, :] = found
        size = jnp.abs(found)
        share = 1.0 / (1.0 + jnp.exp(SHARPNESS * (size - limit)))
        if peak is None:
            peak, shares = size, share
        else:
            peak, shares = jnp.maximum(peak, size), shares + share
    lane = lax.broadcasted_iota(jnp.int32, stats.shape, 1)
    stats[...] = jnp.where(lane == 0, jnp.max(peak), jnp.sum(shares))

    @pl.when(lax.axis_index("ka") == ITERS - 1)
    def _():
        plain = sum(mm(unfold_rows[...], part) for part in reversed(terms(image[...])))
        pack[:tile, :] = sum(mm(part, unfold_cols[...]) for part in reversed(terms(plain)))


def final_body(pack, other, stats, intensity, errors, peaks, shares, *, total):
    tile = pack.shape[1]
    first = lax.axis_index("ka") == 0
    intensity[...] = jnp.where(first, other[:tile, :], pack[:tile, :])
    mine = pack[tile:, :]
    theirs = other[tile:, :]
    zero = jnp.where(first, mine, theirs)
    one = jnp.where(first, theirs, mine)
    for j in range(errors.shape[3] // tile):
        lanes = slice(j * tile, (j + 1) * tile)
        errors[0, 0, 0:1, lanes] = zero[j : j + 1]
        errors[0, 0, 1:2, lanes] = one[j : j + 1]
    got = stats[...]
    iteration = lax.broadcasted_iota(jnp.int32, got.shape, 0) % ITERS
    lane = lax.broadcasted_iota(jnp.int32, got.shape, 1)
    for t in range(ITERS):
        peaks[t] = jnp.max(jnp.where((iteration == t) & (lane == 0), got, 0.0))
        shares[t] = jnp.sum(jnp.where((iteration == t) & (lane == 1), got, 0.0)) / total


def spec(count, space=VMEM):
    return [pl.BlockSpec(memory_space=space)] * count


def in_hbm(x):
    return pltpu.with_memory_space_constraint(x, pltpu.MemorySpace.HBM)


def shape(*dims):
    return jax.ShapeDtypeStruct(dims, F32)


def neighbours(axis, send_a, send_b):
    count = lax.axis_size(axis)
    got = []
    for start, sent in ((0, send_a), (1, send_b)):
        pairs = [(i, i + 1) for i in range(start, count - 1, 2)]
        if pairs:
            got.append(lax.ppermute(sent, axis, pairs + [(b, a) for a, b in pairs]))
        else:
            got.append(jnp.zeros_like(sent))
    return got


def shards(
    mask_raster,
    frag_rows,
    frag_cols,
    frag_length,
    frag_orient,
    frag_moves,
    site_rows,
    site_cols,
    spectra,
    weights,
    tolerance,
):
    tile = mask_raster.shape[0]
    sites = site_rows.shape[2]
    fwd_rows, fwd_cols, expand, inv_rows, inv_cols, unfold = tables(tile)
    half_rows = fwd_rows[0].shape[0]
    swap = [(0, 1), (1, 0)]
    corrected, current, send_a, send_b = pl.pallas_call(
        strips_body,
        out_shape=[shape(tile, tile), shape(tile, tile), shape(HALO, tile), shape(HALO, tile)],
        in_specs=spec(6),
        out_specs=spec(4),
        compiler_params=LIMIT,
        name="strips",
    )(*map(in_hbm, (mask_raster, frag_rows, frag_cols, frag_length, frag_orient, frag_moves)))
    got_a, got_b = neighbours("tx", send_a, send_b)
    scaled, *row_tables = pl.pallas_call(
        functools.partial(prepare_rows_body, count=len(fwd_rows)),
        out_shape=[shape(*spectra.shape)]
        + [jax.ShapeDtypeStruct(c.shape, BF16) for c in fwd_rows],
        in_specs=spec(1, pl.ANY) + spec(1, SMEM) + spec(1 + len(fwd_rows), pl.ANY),
        out_specs=spec(1 + len(fwd_rows)),
        scratch_shapes=[pltpu.SemaphoreType.DMA((1 + len(fwd_rows),))],
        compiler_params=LIMIT,
        name="prepare_rows",
    )(send_a, weights, in_hbm(spectra), *[in_hbm(jnp.asarray(c)) for c in fwd_rows])
    scaled_other = lax.ppermute(scaled, "ka", swap)
    mine, send_a, send_b = pl.pallas_call(
        rows_body,
        out_shape=[shape(half_rows, tile), shape(half_rows, HALO), shape(half_rows, HALO)],
        in_specs=spec(6),
        out_specs=spec(3),
        compiler_params=LIMIT,
        name="rows",
    )(current, got_a, got_b, *row_tables)
    got_a, got_b = neighbours("ty", send_a, send_b)
    constants = [*fwd_cols, expand, *inv_rows, *inv_cols, *unfold]
    chosen, rows_at, limits, *constants = pl.pallas_call(
        functools.partial(prepare_image_body, count=len(constants)),
        out_shape=[
            jax.ShapeDtypeStruct((tile, sites), BF16),
            jax.ShapeDtypeStruct(site_rows.shape, jnp.int32),
            shape(8, 128),
        ]
        + [jax.ShapeDtypeStruct(c.shape, BF16) for c in constants],
        in_specs=spec(1, pl.ANY) + spec(1, SMEM) + spec(2) + spec(len(constants), pl.ANY),
        out_specs=spec(3 + len(constants)),
        scratch_shapes=[pltpu.SemaphoreType.DMA((len(constants),))],
        compiler_params=LIMIT,
        name="prepare_image",
    )(
        send_a,
        tolerance,
        in_hbm(site_rows),
        in_hbm(site_cols),
        *[in_hbm(jnp.asarray(c)) for c in constants],
    )
    members = lax.axis_size("tx") * lax.axis_size("ty") * lax.axis_size("ka")
    pack_rows = tile + sites // tile
    pack, stats = pl.pallas_call(
        image_body,
        out_shape=[shape(pack_rows, tile), shape(members, 128)],
        in_specs=spec(8 + len(constants)),
        out_specs=spec(2),
        scratch_shapes=[pltpu.VMEM((tile, tile), F32)],
        compiler_params=LIMIT,
        name="image",
    )(
        mine,
        got_a,
        got_b,
        scaled,
        scaled_other,
        rows_at,
        chosen,
        limits,
        *constants,
    )
    other = lax.ppermute(pack, "ka", swap)
    merged = lax.all_to_all(stats, ("tx", "ty", "ka"), 0, 0, tiled=True)
    total = float(sites * lax.axis_size("tx") * lax.axis_size("ty"))
    intensity, errors, peaks, shares = pl.pallas_call(
        functools.partial(final_body, total=total),
        out_shape=[shape(tile, tile), shape(1, 1, ITERS, sites), shape(ITERS), shape(ITERS)],
        in_specs=spec(3),
        out_specs=spec(2) + spec(2, SMEM),
        compiler_params=LIMIT,
        name="final",
    )(pack, other, merged)
    return (intensity, corrected, errors, peaks, shares)


def solution(mesh):
    assert mesh.shape["ka"] == ITERS
    placed = (
        P(("groups", "tx"), "ty"),
        P(("groups", "tx"), "ty", None),
        P(("groups", "tx"), "ty", None),
        P(("groups", "tx"), "ty", None),
        P(("groups", "tx"), "ty", None),
        P(("groups", "tx"), "ty", None, None),
        P(("groups", "tx"), "ty", None),
        P(("groups", "tx"), "ty", None),
        P("ka", None, None, None),
        P("ka"),
        P(),
    )
    return jax.shard_map(
        shards,
        mesh=mesh,
        in_specs=placed,
        out_specs=(
            P(("groups", "tx"), "ty"),
            P(("groups", "tx"), "ty"),
            P(("groups", "tx"), "ty", None, None),
            P("groups"),
            P("groups"),
        ),
        check_vma=False,
    )
```

```python
import functools
import math

import jax
import jax.numpy as jnp
import numpy as np
from jax import lax
from jax.experimental import pallas as pl
from jax.experimental.pallas import tpu as pltpu
from jax.sharding import PartitionSpec as P


HALO = 128
BAND = 128
ITERS = 2

LEVEL = 0.4
SLOPE_FLOOR = 0.05
SHARPNESS = 8.0

F32 = jnp.float32
BF16 = jnp.bfloat16
VMEM = pltpu.MemorySpace.VMEM
SMEM = pltpu.MemorySpace.SMEM
PAD_ROWS = 16
LIMIT = pltpu.CompilerParams(vmem_limit_bytes=24 * 1024 * 1024)


def terms(x):
    high = x.astype(BF16)
    rest = x - high.astype(F32)
    mid = rest.astype(BF16)
    return high, mid, (rest - mid.astype(F32)).astype(BF16)


def table_terms(table):
    out = []
    for _ in range(3):
        part = table.astype(np.float32).astype(BF16)
        out.append(part)
        table = table - part.astype(np.float64)
    return out


@functools.lru_cache(maxsize=None)
def tables(tile):
    ext = tile + 2 * HALO
    half = BAND // 2
    rows = (BAND + 1 + PAD_ROWS - 1) // PAD_ROWS * PAD_ROWS
    step = 2.0 * math.pi / ext
    place = np.arange(ext) - (ext - 1) / 2
    freq = np.arange(BAND) - half

    def angle(freqs, places):
        return freqs[:, None] * places[None, :] * step

    forward_rows = np.zeros((rows, ext))
    forward_rows[: half + 1] = np.cos(angle(np.arange(half + 1), place))
    forward_rows[half + 1 : BAND + 1] = -np.sin(angle(np.arange(1, half + 1), place))
    turn = angle(place, freq)
    forward_cols = np.concatenate([np.cos(turn), np.sin(turn)], axis=1)
    expand = np.zeros((2 * BAND, rows))
    for index, f in enumerate(freq):
        expand[index, abs(f)] = 1.0
        if f != 0:
            expand[BAND + index, half + abs(f)] = np.sign(f)
    inner = angle(np.arange(tile // 2) + 0.5, freq)
    high, mid, low = table_terms(np.concatenate([np.cos(inner), np.sin(inner)]) / ext)
    inverse_rows = [np.concatenate(p, axis=1) for p in ((high, high), (mid, mid), (low, high))]
    inverse_cols = [np.ascontiguousarray(part.T) for part in inverse_rows]
    unfold = np.zeros((tile, tile))
    for j in range(tile // 2):
        unfold[tile // 2 + j, j] = 1.0
        unfold[tile // 2 - 1 - j, tile // 2 + j] = 1.0
    unfold = unfold.astype(np.float32).astype(BF16)
    return (
        table_terms(forward_rows),
        table_terms(forward_cols),
        expand.astype(np.float32).astype(BF16),
        inverse_rows,
        inverse_cols,
        [unfold, np.ascontiguousarray(unfold.T)],
    )


def mm(a, b):
    return jnp.dot(a, b, preferred_element_type=F32)


def mm6(a, b):
    small = mm(a[2], b[0]) + mm(a[0], b[2]) + mm(a[1], b[1])
    return small + mm(a[1], b[0]) + mm(a[0], b[1]) + mm(a[0], b[0])


def strip_sum(rows, cols, length, orient, moves, iteration, tile):
    place = lax.broadcasted_iota(jnp.int32, (tile, rows.shape[2]), 0)
    row_start = rows[0]
    col_start = cols[0]
    size = length[0]
    along_rows = orient[0] == 0
    shift = moves[0, 0, iteration : iteration + 1, :]
    lower = jnp.minimum(shift, 0)
    upper = jnp.maximum(shift, 0)
    row_low = jnp.where(along_rows, row_start, row_start + lower)
    row_high = jnp.where(along_rows, row_start + size, row_start + upper)
    col_low = jnp.where(along_rows, col_start + lower, col_start)
    col_high = jnp.where(along_rows, col_start + upper, col_start + size)
    sign = jnp.where(shift > 0, 1.0, jnp.where(shift < 0, -1.0, 0.0))
    in_rows = jnp.where((place >= row_low) & (place < row_high), sign, 0.0)
    in_cols = jnp.where((place >= col_low) & (place < col_high), 1.0, 0.0)
    return lax.dot_general(
        in_rows.astype(BF16),
        in_cols.astype(BF16),
        (((1,), (1,)), ((), ())),
        preferred_element_type=F32,
    )


def strips_body(mask, rows, cols, length, orient, moves, current, send_a, send_b):
    tile = mask.shape[0]
    even = lax.axis_index("tx") % 2 == 0
    frags = (rows, cols, length, orient, moves)
    current[...] = jnp.clip(mask[...] + strip_sum(*frags, 0, tile), 0.0, 1.0)

    @pl.when(lax.axis_index("ka") == ITERS - 1)
    def _():
        current[...] = jnp.clip(current[...] + strip_sum(*frags, 1, tile), 0.0, 1.0)

    top = current[:HALO]
    bottom = current[tile - HALO :]
    send_a[...] = jnp.where(even, bottom, top)
    send_b[...] = jnp.where(even, top, bottom)


def corrected_body(current, anchor, rows, cols, length, orient, moves, corrected):
    tile = current.shape[0]
    corrected[...] = current[...]

    @pl.when(lax.axis_index("ka") == 0)
    def _():
        frags = (rows, cols, length, orient, moves)
        corrected[...] = jnp.clip(current[...] + strip_sum(*frags, 1, tile), 0.0, 1.0)


def prepare_rows_body(anchor, weights, spectra, *refs, count):
    tables_in = refs[:count]
    scaled = refs[count]
    tables_out = refs[count + 1 : 2 * count + 1]
    sems = refs[-1]
    copies = [
        pltpu.make_async_copy(source, target, sems.at[i])
        for i, (source, target) in enumerate(zip([spectra, *tables_in], [scaled, *tables_out]))
    ]
    for copy in copies:
        copy.start()
    copies[0].wait()
    lanes = scaled.shape[3]
    for k in range(scaled.shape[0]):
        factor = jnp.sqrt(jnp.full((1, 1, lanes), weights[k]))
        scaled[k] = scaled[k] * factor
    for copy in copies[1:]:
        copy.wait()


def prepare_image_body(*refs, count):
    _, tolerance, site_rows, site_cols = refs[:4]
    tables_in = refs[4 : 4 + count]
    chosen, rows_out, limits = refs[4 + count : 7 + count]
    tables_out = refs[7 + count : 7 + 2 * count]
    sems = refs[-1]
    copies = [
        pltpu.make_async_copy(source, target, sems.at[i])
        for i, (source, target) in enumerate(zip(tables_in, tables_out))
    ]
    for copy in copies:
        copy.start()
    which = lax.axis_index("ka")
    limits[...] = jnp.full(limits.shape, tolerance[which].astype(F32) / 8.0)
    tile = chosen.shape[0]

    def folded(position):
        return jnp.where(position >= tile // 2, position - tile // 2, tile - 1 - position)

    rows_out[...] = folded(site_rows[...])
    place = lax.broadcasted_iota(jnp.int32, chosen.shape, 0)
    chosen[...] = jnp.where(place == folded(site_cols[0]), 1.0, 0.0).astype(BF16)
    for copy in copies:
        copy.wait()


def rows_body(current, got_a, got_b, high, mid, low, out, send_a, send_b):
    tile = current.shape[1]
    even = lax.axis_index("tx") % 2 == 0
    even_col = lax.axis_index("ty") % 2 == 0
    above = jnp.where(even, got_b[...], got_a[...])
    below = jnp.where(even, got_a[...], got_b[...])
    extended = jnp.concatenate([above, current[...], below], axis=0)
    result = mm6((high[...], mid[...], low[...]), terms(extended))
    out[...] = result
    left = result[:, :HALO]
    right = result[:, tile - HALO :]
    send_a[...] = jnp.where(even_col, right, left)
    send_b[...] = jnp.where(even_col, left, right)


def fold_difference(x, axis):
    half = x.shape[axis] // 2
    sides = (lax.slice_in_dim(x, 0, half, axis=axis), lax.slice_in_dim(x, half, 2 * half, axis=axis))
    out = []
    for side, other in (sides, sides[::-1]):
        first = lax.broadcasted_iota(jnp.int32, side.shape, axis) == 0
        edge = lax.slice_in_dim(other, 0, 1, axis=axis)
        inward = jnp.where(first, edge, pltpu.roll(side, 1, axis))
        out.append(pltpu.roll(side, half - 1, axis) - inward)
    return jnp.concatenate(out, axis=axis)


def image_body(
    mine,
    got_a,
    got_b,
    spec_own,
    spec_other,
    site_rows,
    chosen,
    limits,
    cols_high,
    cols_mid,
    cols_low,
    expand,
    inv_rows_a,
    inv_rows_b,
    inv_rows_c,
    inv_cols_a,
    inv_cols_b,
    inv_cols_c,
    unfold_rows,
    unfold_cols,
    pack,
    stats,
    image,
):
    tile = mine.shape[1]
    half = tile // 2
    even_col = lax.axis_index("ty") % 2 == 0
    left = jnp.where(even_col, got_b[...], got_a[...])
    right = jnp.where(even_col, got_a[...], got_b[...])
    window = jnp.concatenate([left, mine[...], right], axis=1)
    half_spec = terms(mm6(terms(window), (cols_high[...], cols_mid[...], cols_low[...])))
    quads = sum(mm(expand[...], part) for part in reversed(half_spec))
    spec_re = quads[:BAND, :BAND] + quads[BAND:, BAND:]
    spec_im = quads[BAND:, :BAND] - quads[:BAND, BAND:]
    count = spec_own.shape[0]
    image[...] = jnp.zeros(image.shape, F32)

    def add_kernel(spec, k):
        kr = spec[k, 0]
        ki = spec[k, 1]
        product = jnp.concatenate(
            [kr * spec_re - ki * spec_im, kr * spec_im + ki * spec_re], axis=1
        )
        high, mid, low = terms(product)
        first = jnp.concatenate([high, mid], axis=0)
        second = jnp.concatenate([high, low], axis=0)
        inner = mm(inv_rows_c[...], second) + mm(inv_rows_b[...], first) + mm(inv_rows_a[...], first)
        even_re = inner[:half, :BAND]
        even_im = inner[:half, BAND:]
        odd_re = inner[half:, :BAND]
        odd_im = inner[half:, BAND:]
        folded = jnp.concatenate(
            [even_re - odd_im, even_re + odd_im, even_im + odd_re, even_im - odd_re], axis=0
        )
        high, mid, low = terms(folded)
        first = jnp.concatenate([high, mid], axis=1)
        second = jnp.concatenate([high, low], axis=1)
        field = mm(second, inv_cols_c[...]) + mm(first, inv_cols_b[...]) + mm(first, inv_cols_a[...])
        even_re = field[:tile, :half]
        odd_re = field[:tile, half:]
        even_im = field[tile:, :half]
        odd_im = field[tile:, half:]
        forth_re = even_re - odd_im
        forth_im = even_im + odd_re
        back_re = even_re + odd_im
        back_im = even_im - odd_re
        forth = forth_re * forth_re + forth_im * forth_im
        back = back_re * back_re + back_im * back_im
        image[:, :half] += forth
        image[:, half:] += back

    def add_kernels(step, carry):
        for j in range(4):
            add_kernel(spec_own, step * 4 + j)
            add_kernel(spec_other, step * 4 + j)
        return carry

    lax.fori_loop(0, count // 4, add_kernels, 0)
    picture = image[...]
    grad_rows = fold_difference(picture, 0) * 0.5
    grad_cols = fold_difference(picture, 1) * 0.5
    slope = jnp.sqrt(grad_rows * grad_rows + grad_cols * grad_cols)
    errors = terms((picture - LEVEL) / jnp.maximum(slope, SLOPE_FLOOR))
    sites = site_rows.shape[2]
    place = lax.broadcasted_iota(jnp.int32, (tile, tile), 0)
    limit = limits[...][0:1, 0:1]
    peak = None
    for j in range(sites // tile):
        lanes = slice(j * tile, (j + 1) * tile)
        sampled = mm(errors[0], chosen[:, lanes]) + mm(errors[1], chosen[:, lanes])
        found = jnp.sum(
            jnp.where(place == site_rows[0, :, lanes], sampled, 0.0), axis=0, keepdims=True
        )
        pack[tile + j : tile + j + 1, :] = found
        size = jnp.abs(found)
        share = 1.0 / (1.0 + jnp.exp(SHARPNESS * (size - limit)))
        if peak is None:
            peak, shares = size, share
        else:
            peak, shares = jnp.maximum(peak, size), shares + share
    lane = lax.broadcasted_iota(jnp.int32, stats.shape, 1)
    stats[...] = jnp.where(lane == 0, jnp.max(peak), jnp.sum(shares))

    @pl.when(lax.axis_index("ka") == ITERS - 1)
    def _():
        plain = sum(mm(unfold_rows[...], part) for part in reversed(terms(image[...])))
        pack[:tile, :] = sum(mm(part, unfold_cols[...]) for part in reversed(terms(plain)))


def final_body(pack, other, stats, intensity, errors, peaks, shares, *, total):
    tile = pack.shape[1]
    first = lax.axis_index("ka") == 0
    intensity[...] = jnp.where(first, other[:tile, :], pack[:tile, :])
    mine = pack[tile:, :]
    theirs = other[tile:, :]
    zero = jnp.where(first, mine, theirs)
    one = jnp.where(first, theirs, mine)
    for j in range(errors.shape[3] // tile):
        lanes = slice(j * tile, (j + 1) * tile)
        errors[0, 0, 0:1, lanes] = zero[j : j + 1]
        errors[0, 0, 1:2, lanes] = one[j : j + 1]
    got = stats[...]
    iteration = lax.broadcasted_iota(jnp.int32, got.shape, 0) % ITERS
    lane = lax.broadcasted_iota(jnp.int32, got.shape, 1)
    for t in range(ITERS):
        peaks[t] = jnp.max(jnp.where((iteration == t) & (lane == 0), got, 0.0))
        shares[t] = jnp.sum(jnp.where((iteration == t) & (lane == 1), got, 0.0)) / total


def spec(count, space=VMEM):
    return [pl.BlockSpec(memory_space=space)] * count


def in_hbm(x):
    return pltpu.with_memory_space_constraint(x, pltpu.MemorySpace.HBM)


def shape(*dims):
    return jax.ShapeDtypeStruct(dims, F32)


def neighbours(axis, send_a, send_b):
    count = lax.axis_size(axis)
    got = []
    for start, sent in ((0, send_a), (1, send_b)):
        pairs = [(i, i + 1) for i in range(start, count - 1, 2)]
        if pairs:
            got.append(lax.ppermute(sent, axis, pairs + [(b, a) for a, b in pairs]))
        else:
            got.append(jnp.zeros_like(sent))
    return got


def shards(
    mask_raster,
    frag_rows,
    frag_cols,
    frag_length,
    frag_orient,
    frag_moves,
    site_rows,
    site_cols,
    spectra,
    weights,
    tolerance,
):
    tile = mask_raster.shape[0]
    sites = site_rows.shape[2]
    fwd_rows, fwd_cols, expand, inv_rows, inv_cols, unfold = tables(tile)
    half_rows = fwd_rows[0].shape[0]
    swap = [(0, 1), (1, 0)]
    frags = [in_hbm(x) for x in (frag_rows, frag_cols, frag_length, frag_orient, frag_moves)]
    current, send_a, send_b = pl.pallas_call(
        strips_body,
        out_shape=[shape(tile, tile), shape(HALO, tile), shape(HALO, tile)],
        in_specs=spec(6),
        out_specs=spec(3),
        compiler_params=LIMIT,
        name="strips",
    )(in_hbm(mask_raster), *frags)
    corrected = pl.pallas_call(
        corrected_body,
        out_shape=shape(tile, tile),
        in_specs=spec(1) + spec(1, pl.ANY) + spec(5),
        out_specs=spec(1)[0],
        compiler_params=LIMIT,
        name="corrected",
    )(current, send_a, *frags)
    got_a, got_b = neighbours("tx", send_a, send_b)
    scaled, *row_tables = pl.pallas_call(
        functools.partial(prepare_rows_body, count=len(fwd_rows)),
        out_shape=[shape(*spectra.shape)]
        + [jax.ShapeDtypeStruct(c.shape, BF16) for c in fwd_rows],
        in_specs=spec(1, pl.ANY) + spec(1, SMEM) + spec(1 + len(fwd_rows), pl.ANY),
        out_specs=spec(1 + len(fwd_rows)),
        scratch_shapes=[pltpu.SemaphoreType.DMA((1 + len(fwd_rows),))],
        compiler_params=LIMIT,
        name="prepare_rows",
    )(send_a, weights, in_hbm(spectra), *[in_hbm(jnp.asarray(c)) for c in fwd_rows])
    scaled_other = lax.ppermute(scaled, "ka", swap)
    mine, send_a, send_b = pl.pallas_call(
        rows_body,
        out_shape=[shape(half_rows, tile), shape(half_rows, HALO), shape(half_rows, HALO)],
        in_specs=spec(6),
        out_specs=spec(3),
        compiler_params=LIMIT,
        name="rows",
    )(current, got_a, got_b, *row_tables)
    got_a, got_b = neighbours("ty", send_a, send_b)
    constants = [*fwd_cols, expand, *inv_rows, *inv_cols, *unfold]
    chosen, rows_at, limits, *constants = pl.pallas_call(
        functools.partial(prepare_image_body, count=len(constants)),
        out_shape=[
            jax.ShapeDtypeStruct((tile, sites), BF16),
            jax.ShapeDtypeStruct(site_rows.shape, jnp.int32),
            shape(8, 128),
        ]
        + [jax.ShapeDtypeStruct(c.shape, BF16) for c in constants],
        in_specs=spec(1, pl.ANY) + spec(1, SMEM) + spec(2) + spec(len(constants), pl.ANY),
        out_specs=spec(3 + len(constants)),
        scratch_shapes=[pltpu.SemaphoreType.DMA((len(constants),))],
        compiler_params=LIMIT,
        name="prepare_image",
    )(
        send_a,
        tolerance,
        in_hbm(site_rows),
        in_hbm(site_cols),
        *[in_hbm(jnp.asarray(c)) for c in constants],
    )
    members = lax.axis_size("tx") * lax.axis_size("ty") * lax.axis_size("ka")
    pack_rows = tile + sites // tile
    pack, stats = pl.pallas_call(
        image_body,
        out_shape=[shape(pack_rows, tile), shape(members, 128)],
        in_specs=spec(8 + len(constants)),
        out_specs=spec(2),
        scratch_shapes=[pltpu.VMEM((tile, tile), F32)],
        compiler_params=LIMIT,
        name="image",
    )(
        mine,
        got_a,
        got_b,
        scaled,
        scaled_other,
        rows_at,
        chosen,
        limits,
        *constants,
    )
    other = lax.ppermute(pack, "ka", swap)
    merged = lax.all_to_all(stats, ("tx", "ty", "ka"), 0, 0, tiled=True)
    total = float(sites * lax.axis_size("tx") * lax.axis_size("ty"))
    intensity, errors, peaks, shares = pl.pallas_call(
        functools.partial(final_body, total=total),
        out_shape=[shape(tile, tile), shape(1, 1, ITERS, sites), shape(ITERS), shape(ITERS)],
        in_specs=spec(3),
        out_specs=spec(2) + spec(2, SMEM),
        compiler_params=LIMIT,
        name="final",
    )(pack, other, merged)
    return (intensity, corrected, errors, peaks, shares)


def solution(mesh):
    assert mesh.shape["ka"] == ITERS
    placed = (
        P(("groups", "tx"), "ty"),
        P(("groups", "tx"), "ty", None),
        P(("groups", "tx"), "ty", None),
        P(("groups", "tx"), "ty", None),
        P(("groups", "tx"), "ty", None),
        P(("groups", "tx"), "ty", None, None),
        P(("groups", "tx"), "ty", None),
        P(("groups", "tx"), "ty", None),
        P("ka", None, None, None),
        P("ka"),
        P(),
    )
    return jax.shard_map(
        shards,
        mesh=mesh,
        in_specs=placed,
        out_specs=(
            P(("groups", "tx"), "ty"),
            P(("groups", "tx"), "ty"),
            P(("groups", "tx"), "ty", None, None),
            P("groups"),
            P("groups"),
        ),
        check_vma=False,
    )
```
